32 devices in a mesh: groups: 2 (over y), blk: 4 (over z), tok: 4 (over x, core).
Axes of the slice: x: 2, y: 2, z: 4, core: 2. Of those that a mesh axis runs over, the one named last changes fastest.
Arguments:
- tokens: bfloat16 [2048, 3584], P(('groups', 'blk', 'tok')), parts along dimension 0, may hold values from -6 to 6
- expert_ids: int32 [2048, 1], P(('groups', 'blk', 'tok')), parts along dimension 0, may hold values from 0 to 1; in each aligned block of 256 rows (0 to 255, 256 to 511, ...) at most 192 rows name the same one
- gate_values: float32 [2048, 1], P(('groups', 'blk', 'tok')), parts along dimension 0, may hold values from 0.2 to 1
- w_gate: bfloat16 [2, 3584, 1024], P(None, 'blk', 'tok'), may hold values from -0.09375 to 0.09375
- w_up: bfloat16 [2, 3584, 1024], P(None, 'blk', 'tok'), may hold values from -0.09375 to 0.09375
- w_down: bfloat16 [2, 1024, 3584], P(None, 'tok', 'blk'), may hold values from -0.1875 to 0.1875
Outputs:
- mixed: bfloat16 [2048, 3584], P(('groups', 'blk', 'tok')), parts along dimension 0
The draws below stay inside these ranges and needn't reach their ends.
There are 2 independent parts, one for each index of `groups`. The reference program is written for one: setup_inputs(seed, part) draws one part's arguments, and reference() takes and returns one part's arrays. A program takes and returns all parts, laid end to end along the dimension named above; an argument that names none is the same for every part. Nothing has to cross between parts.
Inputs may be any that keep to these rules, and one draw needn't show every extreme that they name: `expert_ids`: in each aligned block of 256 rows (the tokens of one index of blk), no expert is named by more than 192 rows, and in every draw some expert reaches 192 in some block.
All inputs are finite; a program needn't handle non-finite values.
Results may differ from the reference program's by a relative error of at most 0.005.
Values may be sent and summed in bfloat16 or wider, within the bound.
No kernel may reach another device: no remote copies, remote signals or barrier semaphores. Data moves between devices by JAX's collectives and lax.ppermute only.
A program may use at most 64 MiB of HBM per device.

```python
import math
import jax
import jax.numpy as jnp
import numpy as np
from jax import lax

D = 3584
FF = 1024
EXPERTS = 2
TOPK = 1
GROUP = 256
CAP = 192
TOKENS = 1024


def steps_of(key, shape, cuts, least, high):
    def one(axis_at, shards_of):
        heights = jax.random.uniform(jax.random.fold_in(jax.random.fold_in(key, 6), axis_at), (shards_of,), jnp.float32, least / len(cuts), high / len(cuts))
        return jnp.repeat(jnp.exp(heights), shape[axis_at] // shards_of).reshape((-1,) + (1,) * (len(shape) - axis_at - 1))

    gain = one(*cuts[0])
    for cut in cuts[1:]:
        gain = gain * one(*cut)
    return gain


def assign_block(stream_key, own, number, rows, amount, top, reach, slope):
    sequence = jax.random.permutation(stream_key, amount)
    crowded, ordinary = shares(amount, rows * top, reach, slope, True), shares(amount, rows * top, reach, slope, False)
    places = jnp.arange(amount)

    def named(tallies, turn):
        used = int((tallies > 0).sum())
        fixed = max(1, used // 4)
        moved = fixed + (places - fixed + turn * (used - fixed)) % max(1, amount - fixed)
        return jnp.zeros((amount,), jnp.int32).at[sequence[jnp.where(places < fixed, places, moved)]].set(jnp.asarray(tallies, jnp.int32))

    tallies = jnp.where(number % 4 == 0, named(crowded, number // 4), named(ordinary, number - number // 4 - 1))
    mixed = jax.random.permutation(jax.random.fold_in(own, 3), amount)
    source_of, taker = mixed[0:amount // 2 * 2:2], mixed[1:amount // 2 * 2:2]
    margin = jnp.minimum(tallies[source_of] - 1, reach - tallies[taker]) // 2
    margin = jnp.where((source_of == sequence[0]) | (taker == sequence[0]) | (tallies[taker] == 0), 0, jnp.maximum(margin, 0))
    moved = jax.random.randint(jax.random.fold_in(own, 4), (amount // 2,), 0, 1 << 20) % (margin + 1)
    tallies = tallies.at[source_of].add(-moved).at[taker].add(moved)
    labels = jnp.searchsorted(jnp.cumsum(tallies), jnp.arange(rows * top), side="right").astype(jnp.int32)
    listing = labels.reshape(top, rows).T
    listing = listing[jax.random.permutation(jax.random.fold_in(own, 1), rows)]
    turn = jax.random.randint(jax.random.fold_in(own, 2), (rows, 1), 0, top)
    return jnp.take_along_axis(listing, (jnp.arange(top)[None, :] + turn) % top, axis=1)


def shares(amount, total, most, lean, full):
    portions = [(1 << 20) // math.isqrt(rank ** lean) + 1 for rank in range(1, amount + 1)]
    largest = most if full else min(most, max(-(-total // amount), total * portions[0] // sum(portions)))
    least = 1 if total - largest >= amount - 1 else 0
    given, spare = [largest] + [least] * (amount - 1), total - largest - least * (amount - 1)
    while spare > 0:
        candidates = [i for i in range(1, amount) if given[i] < largest] or [i for i in range(1, amount) if given[i] < most]
        whole, budget = sum([portions[i] for i in candidates]), spare
        for i in candidates:
            extra = min(most - given[i], max(1, budget * portions[i] // whole), spare)
            given[i] = given[i] + extra
            spare = spare - extra
    return np.array(given)


def gaussian(stream_key, dims, width, limit, cuts=(), kind=jnp.bfloat16):
    drawn = jax.random.normal(stream_key, dims, jnp.float32) * width
    if len(cuts) > 0:
        drawn = steps_of(stream_key, dims, cuts, -0.22, 0.18) * drawn
    return jnp.clip(drawn, min=-limit, max=limit).astype(kind)


def setup_inputs(seed: int = 0, part: int = 0) -> dict:
    streams_of = jax.random.split(jax.random.key(seed), 7)
    own_keys = jax.random.split(jax.random.fold_in(streams_of[6], part), 7)
    tokens = gaussian(own_keys[0], (TOKENS, D), 1.0, 6.0, ((0, 16),))
    expert_ids_keys = jax.random.split(jax.random.fold_in(own_keys[1], 1), TOKENS // GROUP)
    expert_ids_turns = jax.random.permutation(jax.random.fold_in(own_keys[1], 3), TOKENS // GROUP)
    expert_ids = jax.vmap(lambda own, number: assign_block(jax.random.fold_in(own_keys[1], 2), own, number, GROUP, EXPERTS, TOPK, CAP, 2))(expert_ids_keys, expert_ids_turns).reshape((TOKENS, TOPK))
    gate_values = jnp.clip(0.2 + 0.8 * jax.random.uniform(own_keys[2], (TOKENS, TOPK), jnp.float32) ** steps_of(own_keys[2], (TOKENS, TOPK), ((0, 16),), -0.2, 0.2), 0.2, 1.0)
    w_gate = gaussian(streams_of[3], (EXPERTS, D, FF), D ** -0.5, 0.09375, ((1, 4), (2, 4)))
    w_up = gaussian(streams_of[4], (EXPERTS, D, FF), D ** -0.5, 0.09375, ((1, 4), (2, 4)))
    w_down = gaussian(streams_of[5], (EXPERTS, FF, D), FF ** -0.5, 0.1875, ((1, 4), (2, 4)))
    return {"tokens": tokens, "expert_ids": expert_ids, "gate_values": gate_values, "w_gate": w_gate, "w_up": w_up, "w_down": w_down}


block_rows = 512


def expert_block(token_block, gate_weight, up_weight, down_weight):
    gate = jnp.dot(token_block, gate_weight, preferred_element_type=jnp.float32)
    up = jnp.dot(token_block, up_weight, preferred_element_type=jnp.float32)
    hidden = (jax.nn.silu(gate) * up).astype(jnp.bfloat16)
    return jnp.dot(hidden, down_weight, preferred_element_type=jnp.float32)


def reference(tokens, expert_ids, gate_values, w_gate, w_up, w_down):
    count_tokens = tokens.shape[0]
    routes = expert_ids[:, 0].astype(jnp.int32)
    onehot = (routes[:, None] == jnp.arange(EXPERTS, dtype=jnp.int32)[None, :]).astype(jnp.int32)
    slot_rank = jnp.sum((jnp.cumsum(onehot, axis=0) - onehot) * onehot, axis=1).astype(jnp.int32)
    counts = jnp.sum(onehot, axis=0).astype(jnp.int32)
    padded = ((counts + block_rows - 1) // block_rows) * block_rows
    starts = (jnp.cumsum(padded) - padded).astype(jnp.int32)
    destination = (jnp.take(starts, routes) + slot_rank).astype(jnp.int32)
    num_blocks = (count_tokens + block_rows - 1) // block_rows + EXPERTS
    total_slots = num_blocks * block_rows
    slot_token = jnp.zeros((total_slots,), jnp.int32).at[destination].set(jnp.arange(count_tokens, dtype=jnp.int32))
    block_start = jnp.arange(num_blocks, dtype=jnp.int32) * block_rows
    block_expert = jnp.sum((starts[None, :] <= block_start[:, None]).astype(jnp.int32), axis=1) - 1
    block_expert = jnp.clip(block_expert, 0, EXPERTS - 1).astype(jnp.int32)

    def run_block(args):
        indices, expert = args
        token_block = jnp.take(tokens, indices, axis=0)
        return expert_block(token_block, w_gate[expert], w_up[expert], w_down[expert])

    outputs = lax.map(run_block, (slot_token.reshape(num_blocks, block_rows), block_expert))
    flat_rows = outputs.reshape(total_slots, tokens.shape[1])
    expert_out = jnp.take(flat_rows, destination, axis=0)
    return (gate_values[:, 0:1] * expert_out).astype(jnp.bfloat16)
```

```python
import jax
import jax.numpy as jnp
from jax import lax
from jax.sharding import PartitionSpec as P


def gather_weights(tokens, expert_ids, gate_values, w_gate, w_up, w_down):
    group_rows = lax.all_gather(tokens, "tok", axis=0, tiled=True)
    group_routes = lax.all_gather(expert_ids, "tok", axis=0, tiled=True)[:, 0]
    experts = w_gate.shape[0]
    count_rows = group_rows.shape[0]
    capacity = 3 * count_rows // 4
    expert_range = jnp.arange(experts, dtype=jnp.int32)
    onehot = (group_routes[:, None] == expert_range[None, :]).astype(jnp.int32)
    slot_rank = jnp.sum((jnp.cumsum(onehot, axis=0) - onehot) * onehot, axis=1)
    expert_match = group_routes[None, None, :] == expert_range[:, None, None]
    slot_match = slot_rank[None, None, :] == jnp.arange(capacity, dtype=jnp.int32)[None, :, None]
    dispatch = (expert_match & slot_match).astype(jnp.bfloat16)
    slots = jnp.einsum(
        "esg,gd->esd", dispatch, group_rows, preferred_element_type=jnp.float32
    ).astype(jnp.bfloat16)

    def add_part(weights):
        return jnp.einsum("esd,edf->esf", slots, weights, preferred_element_type=jnp.float32)

    gate_sum = add_part(lax.all_gather(w_gate, "blk", axis=1, tiled=True))
    up_sum = add_part(lax.all_gather(w_up, "blk", axis=1, tiled=True))
    hidden = (jax.nn.silu(gate_sum) * up_sum).astype(jnp.bfloat16)
    slot_out = jnp.einsum(
        "esf,efd->esd",
        hidden,
        lax.all_gather(w_down, "blk", axis=2, tiled=True),
        preferred_element_type=jnp.float32,
    )
    flat_rows = slot_out.reshape(experts * capacity, slot_out.shape[2])
    position = group_routes * capacity + slot_rank
    partial_value = jnp.take(flat_rows, position, axis=0)
    summed = lax.psum_scatter(partial_value, "tok", scatter_dimension=0, tiled=True)
    return (gate_values * summed).astype(jnp.bfloat16)


def move_rows(blks, toks):
    bf16, f32 = jnp.bfloat16, jnp.float32
    levels = [1 << b for b in range(toks.bit_length() - 1)]

    def shift(x, k):
        return lax.ppermute(x, "blk", [(a, (a + k) % blks) for a in range(blks)])

    def swap(x, m):
        return lax.ppermute(x, "tok", [(a, a ^ m) for a in range(toks)])

    def tok_gather(x):
        for m in reversed(levels):
            x = jnp.concatenate([x, swap(x, m)], axis=0)
        return x

    def tok_reduce(x):
        for m in levels:
            half = x.shape[0] // 2
            x = x[:half] + swap(x[half:].astype(bf16), m).astype(f32)
        return x

    def body(tokens, expert_ids, gate_values, w_gate, w_up, w_down):
        rows, features = tokens.shape
        experts, depth, units = w_gate.shape
        here = lax.axis_index("blk")
        expert_range = jnp.arange(experts, dtype=jnp.int32)
        both = jnp.concatenate([w_gate, w_up], axis=2).reshape(experts * depth, 2 * units)
        down = w_down.reshape(experts * units, depth)
        routes = [expert_ids] + [shift(expert_ids, k) for k in range(1, blks)]
        routes = tok_gather(jnp.concatenate(routes, axis=1))

        def column(k):
            return lax.dynamic_slice_in_dim(tokens, (here + k) % blks * depth, depth, 1)

        def routed(x, k):
            match = routes[:, k, None] == expert_range[None, :]
            parts = jnp.where(match[:, :, None], x[:, None, :], jnp.zeros((), x.dtype))
            return parts.reshape(x.shape[0], experts * x.shape[1])

        sent = [column(0)] + [shift(column(k), k) for k in range(1, blks)]
        partial = []
        for k in range(blks):
            x = tok_gather(sent[k])
            partial.append(jnp.dot(routed(x, k), both, preferred_element_type=f32))
        total = partial[0]
        for k in range(1, blks):
            total = total + shift(partial[k].astype(bf16), -k).astype(f32)
        hidden = (jax.nn.silu(total[:, :units]) * total[:, units:]).astype(bf16)
        pieces = []
        for k in range(blks):
            h = hidden if k == 0 else shift(hidden, k)
            y = tok_reduce(jnp.dot(routed(h, k), down, preferred_element_type=f32))
            pieces.append(y if k == 0 else shift(y.astype(bf16), -k).astype(f32))
        out = jnp.zeros((rows, features), bf16)
        for k in range(blks):
            piece = (gate_values * pieces[k]).astype(bf16)
            out = lax.dynamic_update_slice_in_dim(out, piece, (here + k) % blks * depth, 1)
        return out

    return body


def solution(mesh):
    groups, blks, toks = (mesh.shape[a] for a in ("groups", "blk", "tok"))

    def whole(tokens, expert_ids, gate_values, w_gate, w_up, w_down):
        moved_rows = tokens.shape[0] // groups
        weights = w_gate.shape[0] * w_gate.shape[2]
        small = moved_rows < weights and toks & (toks - 1) == 0
        return jax.shard_map(
            move_rows(blks, toks) if small else gather_weights,
            mesh=mesh,
            in_specs=(
                P(("groups", "blk", "tok"), None),
                P(("groups", "blk", "tok"), None),
                P(("groups", "blk", "tok"), None),
                P(None, "blk", "tok"),
                P(None, "blk", "tok"),
                P(None, "tok", "blk"),
            ),
            out_specs=P(("groups", "blk", "tok"), None),
            check_vma=False,
        )(tokens, expert_ids, gate_values, w_gate, w_up, w_down)

    return whole
```

```python
import jax
import jax.numpy as jnp
from jax import lax
from jax.sharding import PartitionSpec as P


def gather_weights(tokens, expert_ids, gate_values, w_gate, w_up, w_down):
    group_rows = lax.all_gather(tokens, "tok", axis=0, tiled=True)
    group_routes = lax.all_gather(expert_ids, "tok", axis=0, tiled=True)[:, 0]
    experts = w_gate.shape[0]
    count_rows = group_rows.shape[0]
    capacity = 3 * count_rows // 4
    expert_range = jnp.arange(experts, dtype=jnp.int32)
    onehot = (group_routes[:, None] == expert_range[None, :]).astype(jnp.int32)
    slot_rank = jnp.sum((jnp.cumsum(onehot, axis=0) - onehot) * onehot, axis=1)
    expert_match = group_routes[None, None, :] == expert_range[:, None, None]
    slot_match = slot_rank[None, None, :] == jnp.arange(capacity, dtype=jnp.int32)[None, :, None]
    dispatch = (expert_match & slot_match).astype(jnp.bfloat16)
    slots = jnp.einsum(
        "esg,gd->esd", dispatch, group_rows, preferred_element_type=jnp.float32
    ).astype(jnp.bfloat16)

    def add_part(weights):
        return jnp.einsum("esd,edf->esf", slots, weights, preferred_element_type=jnp.float32)

    gate_sum = add_part(lax.all_gather(w_gate, "blk", axis=1, tiled=True))
    up_sum = add_part(lax.all_gather(w_up, "blk", axis=1, tiled=True))
    hidden = (jax.nn.silu(gate_sum) * up_sum).astype(jnp.bfloat16)
    slot_out = jnp.einsum(
        "esf,efd->esd",
        hidden,
        lax.all_gather(w_down, "blk", axis=2, tiled=True),
        preferred_element_type=jnp.float32,
    )
    flat_rows = slot_out.reshape(experts * capacity, slot_out.shape[2])
    position = group_routes * capacity + slot_rank
    partial_value = jnp.take(flat_rows, position, axis=0)
    summed = lax.psum_scatter(partial_value, "tok", scatter_dimension=0, tiled=True)
    return (gate_values * summed).astype(jnp.bfloat16)


def move_rows(blks, toks):
    bf16, f32 = jnp.bfloat16, jnp.float32
    pair = 1 if toks > 1 else 0
    levels = [1 << b for b in range(pair, toks.bit_length() - 1)]
    order = list(range(2, blks)) + list(range(1, min(2, blks)))

    def cross(x, k):
        return lax.ppermute(x, "blk", [(a, a ^ k) for a in range(blks)])

    def swap(x, m):
        return lax.ppermute(x, "tok", [(a, a ^ m) for a in range(toks)])

    def tok_gather(x):
        for m in reversed(levels):
            x = jnp.concatenate([x, swap(x, m)], axis=0)
        return x

    def tok_reduce(x):
        for m in levels:
            half = x.shape[0] // 2
            x = x[:half] + swap(x[half:].astype(bf16), m).astype(f32)
        return x

    def paired(w):
        return [w, swap(w, 1)] if pair else [w]

    def rounded(x):
        return lax.reduce_precision(x, exponent_bits=8, mantissa_bits=7)

    def layer(tokens, expert_ids, gate_values, w_gate, w_up, w_down):
        rows, features = tokens.shape
        experts, depth, _ = w_gate.shape
        here = lax.axis_index("blk")
        high = rounded(gate_values)
        middle = rounded(gate_values - high)
        low = gate_values - high - middle
        lane = lax.broadcasted_iota(jnp.int32, (rows, 128), 1)
        label = jnp.zeros((rows, 128), f32)
        for at, term in enumerate((expert_ids.astype(f32), high, middle, low)):
            label = jnp.where(lane == at, term, label)
        label = label.astype(bf16)

        def column(k):
            part = lax.dynamic_slice_in_dim(tokens, (here ^ k) * depth, depth, 1)
            return jnp.concatenate([part, label], axis=1)

        sent = {k: cross(column(k), k) for k in order}
        sent[0] = column(0)
        gates, ups = paired(w_gate), paired(w_up)
        both = jnp.concatenate(gates + ups, axis=2)
        wide = both.shape[2] // 2
        both = both.reshape(experts * depth, 2 * wide)
        down = jnp.concatenate(paired(w_down), axis=1).reshape(experts * wide, depth)

        def routed(x, route):
            match = [jnp.where(route == e, x, jnp.zeros((), x.dtype)) for e in range(experts)]
            return jnp.concatenate(match, axis=1)

        total, route = None, {}
        for k in order + [0]:
            x = tok_gather(sent[k])
            route[k] = x[:, depth : depth + 1]
            part = jnp.dot(routed(x[:, :depth], route[k]), both, preferred_element_type=f32)
            if k:
                part = cross(part.astype(bf16), k).astype(f32)
            else:
                part = lax.optimization_barrier(part)
            total = part if total is None else total + part
        hidden = (jax.nn.silu(total[:, :wide]) * total[:, wide:]).astype(bf16)
        moved = {k: cross(hidden, k) for k in order}
        moved[0] = hidden
        out = jnp.zeros((rows, features), bf16)
        for k in [0, 1] + order[:-1] if blks > 1 else [0]:
            y = jnp.dot(routed(moved[k], route[k]), down, preferred_element_type=f32)
            y = tok_reduce(y)
            terms = sent[k][:, depth + 1 : depth + 4].astype(f32)
            y = ((terms[:, 0:1] + terms[:, 1:2] + terms[:, 2:3]) * y).astype(bf16)
            if k:
                y = cross(y, k)
            out = lax.dynamic_update_slice_in_dim(out, y, (here ^ k) * depth, 1)
        return out

    return layer


def solution(mesh):
    groups, blks, toks = (mesh.shape[a] for a in ("groups", "blk", "tok"))

    def whole(tokens, expert_ids, gate_values, w_gate, w_up, w_down):
        moved_rows = tokens.shape[0] // groups
        weights = w_gate.shape[0] * w_gate.shape[2]
        powers = toks & (toks - 1) == 0 and blks & (blks - 1) == 0
        small = moved_rows < weights and powers
        step = jax.shard_map(
            move_rows(blks, toks) if small else gather_weights,
            mesh=mesh,
            in_specs=(
                P(("groups", "blk", "tok"), None),
                P(("groups", "blk", "tok"), None),
                P(("groups", "blk", "tok"), None),
                P(None, "blk", "tok"),
                P(None, "blk", "tok"),
                P(None, "tok", "blk"),
            ),
            out_specs=P(("groups", "blk", "tok"), None),
            check_vma=False,
        )
        return step(tokens, expert_ids, gate_values, w_gate, w_up, w_down)

    return whole
```
